128 devices in a mesh: shard: 32 (over y, x, core), tp: 4 (over z).
Axes of the slice: x: 4, y: 4, z: 4, core: 2. Of those that a mesh axis runs over, the one named last changes fastest.
Arguments:
- weight_gate: bfloat16 [2560, 9728], P('shard', 'tp'), may hold values from -0.21875 to 0.21875
- low_gate: bfloat16 [2560, 32], P('shard'), may hold values from -0.125 to 0.125
- high_gate: bfloat16 [32, 9728], P(None, 'tp'), may hold values from -1 to 1
- weight_up: bfloat16 [2560, 9728], P('shard', 'tp'), may hold values from -0.21875 to 0.21875
- low_up: bfloat16 [2560, 32], P('shard'), may hold values from -0.125 to 0.125
- high_up: bfloat16 [32, 9728], P(None, 'tp'), may hold values from -1 to 1
- norm_gain: float32 [2560], P('shard'), may hold values from 0.25 to 1.75
Outputs:
- ready_gate: bfloat16 [2560, 9728], P(None, 'tp')
- ready_up: bfloat16 [2560, 9728], P(None, 'tp')
- factor_gate: float32 [9728], P('tp')
- factor_up: float32 [9728], P('tp')
The draws below stay inside these ranges and needn't reach their ends.
All inputs are finite; a program needn't handle non-finite values.
Results may differ from the reference program's by a relative error of at most 0.001.
Values may be sent and summed in bfloat16 or wider, within the bound.
No kernel may reach another device: no remote copies, remote signals or barrier semaphores. Data moves between devices by JAX's collectives and lax.ppermute only.
A program may use at most 128 MiB of HBM per device.

```python
import jax
import jax.numpy as jnp
from jax import lax

D_MODEL = 2560
D_INNER = 9728
RANK = 32


def spiked(result, rng, source, target, shards_of, factor):
    owner, partner = [(jnp.arange(result.shape[dim]) // (result.shape[dim] // shards_of)).reshape([-1 if axis == dim else 1 for axis in range(result.ndim)]) for dim in (source, target)]
    chosen = jax.random.permutation(rng, shards_of)[partner]
    strong = (owner == chosen) | (owner == (partner + shards_of // 2) % shards_of)
    return jnp.where(strong, factor * result, result)


def block_scale(stream_key, dims, split, low, largest):
    loudness, own = 1.0, jax.random.fold_in(stream_key, 6)
    for position, shards_of in split:
        draws = jnp.exp(jax.random.uniform(jax.random.fold_in(own, position), (shards_of,), jnp.float32, low / len(split), largest / len(split)))
        loudness = loudness * jnp.repeat(draws, dims[position] // shards_of).reshape([-1 if axis == position else 1 for axis in range(len(dims))])
    return loudness


def scatter_about(rng, shape, scale, most, shards=(), dtype=jnp.bfloat16):
    drawn = jax.random.normal(rng, shape, jnp.float32) * scale
    if len(shards) > 0:
        drawn = block_scale(rng, shape, shards, -0.22, 0.18) * drawn
    return jnp.clip(drawn, min=-most, max=most).astype(dtype)


def bell_draw_with(key, shape, scale, bound, shards, heavy, kind=jnp.bfloat16):
    array = scale * jax.random.normal(key, shape, jnp.float32)
    if shards:
        array = array * block_scale(key, shape, shards, -0.22, 0.18)
    return jnp.clip(spiked(array, jax.random.fold_in(key, 3), *heavy), -bound, bound).astype(kind)


def setup_inputs(seed: int = 0) -> dict:
    streams_of = jax.random.split(jax.random.key(seed), 8)
    return {
        "weight_gate": bell_draw_with(streams_of[0], (D_MODEL, D_INNER), D_MODEL ** -0.5, 0.21875, ((0, 32), (1, 4)), (0, 1, 32, 2.75)),
        "low_gate": scatter_about(streams_of[1], (D_MODEL, RANK), D_MODEL ** -0.5, 0.125, ((0, 32),)),
        "high_gate": scatter_about(streams_of[2], (RANK, D_INNER), RANK ** -0.5, 1.0, ((1, 4),)),
        "weight_up": bell_draw_with(streams_of[3], (D_MODEL, D_INNER), D_MODEL ** -0.5, 0.21875, ((0, 32), (1, 4)), (0, 1, 32, 2.75)),
        "low_up": scatter_about(streams_of[4], (D_MODEL, RANK), D_MODEL ** -0.5, 0.125, ((0, 32),)),
        "high_up": scatter_about(streams_of[5], (RANK, D_INNER), RANK ** -0.5, 1.0, ((1, 4),)),
        "norm_gain": jnp.clip(1.0 + 0.15 * jax.random.normal(streams_of[6], (D_MODEL,), jnp.float32), 0.25, 1.75),
    }


mix_rate = 2.0

def reference(weight_gate, low_gate, high_gate, weight_up, low_up, high_up, norm_gain):
    latest_gate = weight_gate.astype(jnp.float32) + mix_rate * jnp.dot(low_gate, high_gate, preferred_element_type=jnp.float32)
    latest_up = weight_up.astype(jnp.float32) + mix_rate * jnp.dot(low_up, high_up, preferred_element_type=jnp.float32)
    latest_gained_gate = latest_gate * norm_gain[:, None]
    latest_gained_up = latest_up * norm_gain[:, None]
    factor_gate = jnp.sqrt(lax.optimization_barrier(jnp.sum(latest_gained_gate * latest_gained_gate, axis=0)))
    ready_gate = (latest_gained_gate / factor_gate).astype(jnp.bfloat16)
    factor_up = jnp.sqrt(lax.optimization_barrier(jnp.sum(latest_gained_up * latest_gained_up, axis=0)))
    ready_up = (latest_gained_up / factor_up).astype(jnp.bfloat16)
    return (ready_gate, ready_up, factor_gate, factor_up)
```

```python
import functools

import jax
import jax.numpy as jnp
from jax import lax
from jax.experimental import pallas as pl
from jax.experimental.pallas import tpu as pltpu
from jax.sharding import PartitionSpec as P


ROWS = 80
HALF = 2432
WIDE = 2 * HALF
FULL = WIDE + 128
TILE = 256
KIB = 1024
RANK = 32
TOP = 48
mix_rate = 2.0


def shard_of(y, x, c):
    return ((y % 4) * 4 + x % 4) * 2 + c


def hops(core0, core1, flip=0):
    step = (core0, core1)
    return [
        (shard_of(y, x, c), shard_of(y + step[c][0], x + step[c][1], c ^ flip))
        for y in range(4)
        for x in range(4)
        for c in range(2)
    ]


FIRST = {1: hops((0, 1), (1, 0)), -1: hops((0, -1), (-1, 0))}
SECOND = {1: hops((1, 0), (0, 1)), -1: hops((-1, 0), (0, -1))}
SIDE = hops((0, 0), (0, 0), 1)
ALONG_X = {d: hops((0, d), (0, d)) for d in (1, -1, 2)}
ALONG_Y = {d: hops((d, 0), (d, 0)) for d in (1, -1, 2)}


def source(first, second, flip):
    me = lax.axis_index("shard")
    core, x, y = (me & 1) ^ flip, (me >> 1) & 3, me >> 3
    sx = (x + jnp.where(core == 0, first, second)) & 3
    sy = (y + jnp.where(core == 0, second, first)) & 3
    return ((sy << 2) + sx) * 2 + core


def sent(array, pairs):
    return lax.ppermute(array, "shard", pairs)


def in_vmem(n):
    return [pl.BlockSpec(memory_space=pltpu.VMEM)] * n


def pack_kernel(gate, up, low_gate_t, low_up_t, gain, high_gate, high_up, block, high, low_v, gain_v, side, sems):
    moves = (
        (low_gate_t, low_v.at[0]),
        (low_up_t, low_v.at[1]),
        (gain, gain_v),
        (gate, block.at[:, pl.ds(0, HALF)]),
        (up, block.at[:, pl.ds(HALF, HALF)]),
        (high_gate, high.at[pl.ds(0, RANK), pl.ds(0, HALF)]),
        (high_up, high.at[pl.ds(RANK, RANK), pl.ds(HALF, HALF)]),
    )
    copies = [pltpu.make_async_copy(src, dst, sems.at[k]) for k, (src, dst) in enumerate(moves)]
    for copy in copies:
        copy.start()
    high[0:RANK, HALF:] = jnp.zeros((RANK, HALF), jnp.bfloat16)
    high[RANK : 2 * RANK, :HALF] = jnp.zeros((RANK, HALF), jnp.bfloat16)
    side[...] = jnp.zeros_like(side)
    for copy in copies[:3]:
        copy.wait()
    g = gain_v[...]
    hi = g.astype(jnp.bfloat16).astype(jnp.float32)
    mid = (g - hi).astype(jnp.bfloat16).astype(jnp.float32)
    side[0:32, 0:ROWS] = low_v[0].astype(jnp.float32) * mix_rate
    side[32:64, 0:ROWS] = low_v[1].astype(jnp.float32) * mix_rate
    side[64:65, 0:ROWS] = hi
    side[65:66, 0:ROWS] = mid
    side[66:67, 0:ROWS] = g - hi - mid
    block[:, WIDE:] = side[...].T[0:ROWS].astype(jnp.bfloat16)
    for copy in copies[3:]:
        copy.wait()


def gain_of(extra):
    row = lax.broadcasted_iota(jnp.int32, (128, 128), 0)
    ones = jnp.where((row >= 64) & (row < 67), 1.0, 0.0).astype(jnp.bfloat16)
    g = jnp.dot(extra, ones, preferred_element_type=jnp.float32)
    return jnp.concatenate([g, g], axis=1)


def sums_kernel(block, high, sums):
    extra = block[:, WIDE:]
    gain = gain_of(extra)
    for j in range(WIDE // TILE):
        cols = pl.ds(j * TILE, TILE)
        v = block[:, cols].astype(jnp.float32) + jnp.dot(
            extra[:, :64], high[:, cols], preferred_element_type=jnp.float32
        )
        v = v * gain
        sums[:, cols] = jnp.sum(v * v, axis=0, keepdims=True)


def add_kernel(a, b, total):
    total[...] = a[...] + b[...]


def ring_kernel(bit, own, plus, minus, far, *outs):
    even = ((lax.axis_index("shard") >> bit) & 1) == 0
    p, m = plus[...], minus[...]
    partner, other = jnp.where(even, m, p), jnp.where(even, p, m)
    total = (own[...] + partner) + (other + far[...])
    if len(outs) == 1:
        outs[0][...] = total
        return
    factor = jnp.sqrt(total)
    outs[0][...] = factor
    outs[1][...] = 1.0 / factor


def halves_kernel(a, b, top, bottom):
    top[...] = a[:TOP]
    bottom[...] = b[TOP:]


def joined_kernel(top, bottom, block):
    block[:TOP] = top[...]
    block[TOP:] = bottom[...]


def merge_kernel(mine, theirs, *refs):
    n, place = len(mine), len(theirs)
    blocks, refs = refs[:n], refs[n:]
    high, inv = refs[0], refs[1]
    moved, refs = refs[2 : 2 + (place > 0)], refs[2 + (place > 0) :]
    out_gate, out_up, ready, sems = refs[2:]
    outs = (out_gate, out_up)
    copies = []

    def send(src, at, flip, h):
        row = pl.multiple_of(source(*at, flip) * ROWS, ROWS)
        copy = pltpu.make_async_copy(
            src.at[:, pl.ds(h * HALF, HALF)],
            outs[h].at[pl.ds(row, ROWS), :],
            sems.at[len(copies)],
        )
        copy.start()
        copies.append(copy)

    for k in range(place):
        for h in range(2):
            send(moved[0].at[k], theirs[k], 1, h)
    extra = jnp.concatenate([b[:, WIDE:] for b in blocks], axis=0)
    gain = gain_of(extra)
    for j in range(WIDE // TILE):
        cols = pl.ds(j * TILE, TILE)
        low_rank = jnp.dot(extra[:, :64], high[:, cols], preferred_element_type=jnp.float32)
        scale = inv[:, cols]
        for k in range(n):
            rows = slice(k * ROWS, (k + 1) * ROWS)
            v = blocks[k][:, cols].astype(jnp.float32) + low_rank[rows]
            ready[k, :, cols] = (v * gain[rows] * scale).astype(jnp.bfloat16)
        if j == HALF // TILE:
            for k in range(n):
                send(ready.at[k], mine[k], 0, 0)
    for k in range(n):
        send(ready.at[k], mine[k], 0, 1)
    for copy in copies:
        copy.wait()


def place_kernel(theirs, *refs):
    moved, refs = refs[: len(theirs)], refs[len(theirs) + 2 :]
    outs, sems = refs[:2], refs[2]
    copies = []
    for i, pair in enumerate(theirs):
        for k, at in enumerate(pair):
            row = pl.multiple_of(source(*at, 1) * ROWS, ROWS)
            for h, out in enumerate(outs):
                copy = pltpu.make_async_copy(
                    moved[i].at[k, :, pl.ds(h * HALF, HALF)],
                    out.at[pl.ds(row, ROWS), :],
                    sems.at[len(copies)],
                )
                copy.start()
                copies.append(copy)
    for copy in copies:
        copy.wait()


OUT = jax.ShapeDtypeStruct((32 * ROWS, HALF), jnp.bfloat16)
ANY = pl.BlockSpec(memory_space=pl.ANY)


def params(mib):
    return pltpu.CompilerParams(vmem_limit_bytes=int(mib * KIB * KIB))


def cost(us):
    return pl.CostEstimate(flops=int(us * 1e3 * 4000), bytes_accessed=1, transcendentals=0)


def small(body, outs, mib, *operands, scratch=(), specs=None):
    return pl.pallas_call(
        body,
        out_shape=outs,
        in_specs=specs or in_vmem(len(operands)),
        out_specs=jax.tree.map(lambda _: pl.BlockSpec(memory_space=pltpu.VMEM), outs),
        scratch_shapes=scratch,
        compiler_params=params(mib),
        cost_estimate=cost(1.0),
    )(*operands)


def merged(blocks, mine, theirs, high, inv, moved, outs):
    operands = [*blocks, high, inv, *moved]
    count = len(operands)
    aliases = {}
    specs = in_vmem(count)
    if outs is None:
        outs = ()

        def body(*refs):
            merge_kernel(mine, theirs, *refs[:count], None, None, *refs[count:])
    else:
        aliases = {count: 0, count + 1: 1}
        specs = specs + [ANY, ANY]
        body = functools.partial(merge_kernel, mine, theirs)
    n = len(mine)
    return pl.pallas_call(
        body,
        out_shape=(OUT, OUT, jax.ShapeDtypeStruct((n, ROWS, WIDE), jnp.bfloat16)),
        in_specs=specs,
        out_specs=(ANY, ANY, pl.BlockSpec(memory_space=pltpu.VMEM)),
        scratch_shapes=[pltpu.SemaphoreType.DMA((2 * (n + len(theirs)),))],
        input_output_aliases=aliases,
        compiler_params=params(14),
        cost_estimate=cost(1.5),
    )(*operands, *outs)


def placed(theirs, moved, outs):
    n = len(moved)
    return pl.pallas_call(
        functools.partial(place_kernel, theirs),
        out_shape=(OUT, OUT),
        in_specs=in_vmem(n) + [ANY, ANY],
        out_specs=(ANY, ANY),
        scratch_shapes=[pltpu.SemaphoreType.DMA((2 * sum(map(len, theirs)),))],
        input_output_aliases={n: 0, n + 1: 1},
        compiler_params=params(10),
        cost_estimate=cost(1.0),
    )(*moved, *outs)


def program(weight_gate, low_gate, high_gate, weight_up, low_up, high_up, norm_gain):
    hbm = pl.BlockSpec(memory_space=pltpu.HBM)
    shape = jax.ShapeDtypeStruct
    a_block = shape((ROWS, FULL), jnp.bfloat16)
    a_sum = shape((1, WIDE), jnp.float32)
    block, high = small(
        pack_kernel,
        (a_block, shape((2 * RANK, WIDE), jnp.bfloat16)),
        62.4,
        weight_gate,
        weight_up,
        low_gate.T,
        low_up.T,
        norm_gain.reshape(1, ROWS),
        high_gate,
        high_up,
        specs=[hbm] * 7,
        scratch=[
            pltpu.VMEM((2, RANK, ROWS), jnp.bfloat16),
            pltpu.VMEM((1, ROWS), jnp.float32),
            pltpu.VMEM((128, 128), jnp.float32),
            pltpu.SemaphoreType.DMA((7,)),
        ],
    )
    held = {(0, 0): block}
    for step in (1, -1):
        held[-step, 0] = sent(block, FIRST[step])
    for step in (1, -1):
        held[0, -step] = sent(block, SECOND[step])

    sums = small(sums_kernel, a_sum, 6, block, high)
    total = small(add_kernel, a_sum, 2, sums, sent(sums, SIDE))
    for axis, along, bit in (("x", ALONG_X, 1), ("y", ALONG_Y, 3)):
        others = [sent(total, along[d]) for d in (1, -1, 2)]
        total = small(
            functools.partial(ring_kernel, bit),
            a_sum if axis == "x" else (a_sum, a_sum),
            2,
            total,
            *others,
        )
    factor, inv = total

    top, bottom = small(
        halves_kernel,
        (shape((TOP, FULL), jnp.bfloat16), shape((ROWS - TOP, FULL), jnp.bfloat16)),
        6,
        held[-1, 0],
        held[1, 0],
    )
    top, bottom = sent(top, FIRST[1]), sent(bottom, FIRST[-1])
    held[2, 0] = small(joined_kernel, a_block, 6, top, bottom)

    for step, order in ((1, (-1, 1, 2)), (-1, (1, -1, 2))):
        for f in order:
            held[f, -step] = sent(held[f, 0], SECOND[step])
    for step, order in ((1, (0, -1)), (-1, (1, 2))):
        for f in order:
            held[f, 2] = sent(held[f, -step], SECOND[step])

    pairs = (
        ((0, 0), (-1, 0)),
        ((0, -1), (0, 1)),
        ((1, 0), (2, 0)),
        ((-1, -1), (1, 1)),
        ((1, -1), (-1, 1)),
        ((2, -1), (2, 1)),
        ((0, 2), (1, 2)),
        ((-1, 2), (2, 2)),
    )
    outs, moved = None, []
    for k, pair in enumerate(pairs):
        late = k - 2
        *outs, ready = merged(
            [held[p] for p in pair],
            pair,
            pairs[late] if late >= 0 else (),
            high,
            inv,
            [moved[late]] if late >= 0 else [],
            outs,
        )
        moved.append(sent(ready, SIDE))
    ready_gate, ready_up = placed(pairs[-2:], moved[-2:], outs)
    factor = factor.reshape(WIDE)
    return ready_gate, ready_up, factor[:HALF], factor[HALF:]


def solution(mesh):
    in_specs = (
        P("shard", "tp"),
        P("shard", None),
        P(None, "tp"),
        P("shard", "tp"),
        P("shard", None),
        P(None, "tp"),
        P("shard"),
    )
    out_specs = (P(None, "tp"), P(None, "tp"), P("tp"), P("tp"))
    return jax.shard_map(program, mesh=mesh, in_specs=in_specs, out_specs=out_specs, check_vma=False)
```

```python
import functools

import jax
import jax.numpy as jnp
from jax import lax
from jax.experimental import pallas as pl
from jax.experimental.pallas import tpu as pltpu
from jax.sharding import PartitionSpec as P


ROWS = 80
HALF = 2432
WIDE = 2 * HALF
FULL = WIDE + 128
TILE = 256
KIB = 1024
RANK = 32
TOP = 48
mix_rate = 2.0


def shard_of(y, x, c):
    return ((y % 4) * 4 + x % 4) * 2 + c


def hops(core0, core1, flip=0):
    step = (core0, core1)
    return [
        (shard_of(y, x, c), shard_of(y + step[c][0], x + step[c][1], c ^ flip))
        for y in range(4)
        for x in range(4)
        for c in range(2)
    ]


FIRST = {d: hops((0, d), (d, 0)) for d in (1, -1, 2)}
SECOND = {d: hops((d, 0), (0, d)) for d in (1, -1, 2)}
SIDE = hops((0, 0), (0, 0), 1)


def source(first, second, flip):
    me = lax.axis_index("shard")
    core, x, y = (me & 1) ^ flip, (me >> 1) & 3, me >> 3
    sx = (x + jnp.where(core == 0, first, second)) & 3
    sy = (y + jnp.where(core == 0, second, first)) & 3
    return ((sy << 2) + sx) * 2 + core


def sent(array, pairs):
    return lax.ppermute(array, "shard", pairs)


def in_vmem(n):
    return [pl.BlockSpec(memory_space=pltpu.VMEM)] * n


def pack_kernel(gate, up, low_gate_t, low_up_t, gain, high_gate, high_up, block, high, low_v, gain_v, side, sems):
    moves = (
        (low_gate_t, low_v.at[0]),
        (low_up_t, low_v.at[1]),
        (gain, gain_v),
        (gate, block.at[:, pl.ds(0, HALF)]),
        (up, block.at[:, pl.ds(HALF, HALF)]),
        (high_gate, high.at[pl.ds(0, RANK), pl.ds(0, HALF)]),
        (high_up, high.at[pl.ds(RANK, RANK), pl.ds(HALF, HALF)]),
    )
    copies = [pltpu.make_async_copy(src, dst, sems.at[k]) for k, (src, dst) in enumerate(moves)]
    for copy in copies:
        copy.start()
    high[0:RANK, HALF:] = jnp.zeros((RANK, HALF), jnp.bfloat16)
    high[RANK : 2 * RANK, :HALF] = jnp.zeros((RANK, HALF), jnp.bfloat16)
    side[...] = jnp.zeros_like(side)
    for copy in copies[:3]:
        copy.wait()
    g = gain_v[...]
    hi = g.astype(jnp.bfloat16).astype(jnp.float32)
    mid = (g - hi).astype(jnp.bfloat16).astype(jnp.float32)
    side[0:32, 0:ROWS] = low_v[0].astype(jnp.float32) * mix_rate
    side[32:64, 0:ROWS] = low_v[1].astype(jnp.float32) * mix_rate
    side[64:65, 0:ROWS] = hi
    side[65:66, 0:ROWS] = mid
    side[66:67, 0:ROWS] = g - hi - mid
    block[:, WIDE:] = side[...].T[0:ROWS].astype(jnp.bfloat16)
    for copy in copies[3:]:
        copy.wait()


def gain_of(extra):
    row = lax.broadcasted_iota(jnp.int32, (128, 128), 0)
    ones = jnp.where((row >= 64) & (row < 67), 1.0, 0.0).astype(jnp.bfloat16)
    g = jnp.dot(extra, ones, preferred_element_type=jnp.float32)
    return jnp.concatenate([g, g], axis=1)


def sums_kernel(block, high, sums):
    extra = block[:, WIDE:]
    gain = gain_of(extra)
    for j in range(WIDE // TILE):
        cols = pl.ds(j * TILE, TILE)
        v = block[:, cols].astype(jnp.float32) + jnp.dot(
            extra[:, :64], high[:, cols], preferred_element_type=jnp.float32
        )
        v = v * gain
        sums[:, cols] = jnp.sum(v * v, axis=0, keepdims=True)


def ring_kernel(bits, own, plus, minus, far, total):
    me = lax.axis_index("shard")
    bit = jnp.where((me & 1) == 0, bits[0], bits[1])
    even = ((me >> bit) & 1) == 0
    p, m = plus[...], minus[...]
    partner, other = jnp.where(even, m, p), jnp.where(even, p, m)
    total[...] = (own[...] + partner) + (other + far[...])


def factor_kernel(mine, theirs, factor, inv):
    root = jnp.sqrt(mine[...] + theirs[...])
    factor[...] = root
    inv[...] = 1.0 / root


def halves_kernel(a, b, top, bottom):
    top[...] = a[:TOP]
    bottom[...] = b[TOP:]


def joined_kernel(top, bottom, block):
    block[:TOP] = top[...]
    block[TOP:] = bottom[...]


def placer(outs, sems, copies):
    def send(src, at, start, flip, h):
        count = src.shape[0]
        row = pl.multiple_of(source(*at, flip) * ROWS + start, 16)
        copy = pltpu.make_async_copy(
            src.at[:, pl.ds(h * HALF, HALF)],
            outs[h].at[pl.ds(row, count), :],
            sems.at[len(copies)],
        )
        copy.start()
        copies.append(copy)

    return send


def merge_kernel(mine, start, theirs, *refs):
    n, place = len(mine), len(theirs)
    blocks, refs = refs[:n], refs[n:]
    high, inv = refs[0], refs[1]
    moved, refs = refs[2 : 2 + place], refs[2 + place :]
    out_gate, out_up, ready, sems = refs[2:]
    count = ready.shape[1]
    copies = []
    send = placer((out_gate, out_up), sems, copies)
    for (pair, first), ref in zip(theirs, moved):
        for k, at in enumerate(pair):
            for h in range(2):
                send(ref.at[k], at, first, 1, h)
    extra = jnp.concatenate([b[:, WIDE:] for b in blocks], axis=0)
    gain = gain_of(extra)
    for j in range(WIDE // TILE):
        cols = pl.ds(j * TILE, TILE)
        low_rank = jnp.dot(extra[:, :64], high[:, cols], preferred_element_type=jnp.float32)
        scale = inv[:, cols]
        for k in range(n):
            rows = slice(k * count, (k + 1) * count)
            v = blocks[k][:, cols].astype(jnp.float32) + low_rank[rows]
            ready[k, :, cols] = (v * gain[rows] * scale).astype(jnp.bfloat16)
        if j == HALF // TILE:
            for k in range(n):
                send(ready.at[k], mine[k], start, 0, 0)
    for k in range(n):
        send(ready.at[k], mine[k], start, 0, 1)
    for copy in copies:
        copy.wait()


def place_kernel(theirs, *refs):
    moved, refs = refs[: len(theirs)], refs[len(theirs) + 2 :]
    copies = []
    send = placer(refs[:2], refs[2], copies)
    for (pair, first), ref in zip(theirs, moved):
        for k, at in enumerate(pair):
            for h in range(2):
                send(ref.at[k], at, first, 1, h)
    for copy in copies:
        copy.wait()


OUT = jax.ShapeDtypeStruct((32 * ROWS, HALF), jnp.bfloat16)
ANY = pl.BlockSpec(memory_space=pl.ANY)


def params(mib):
    return pltpu.CompilerParams(vmem_limit_bytes=int(mib * KIB * KIB))


def cost(us):
    return pl.CostEstimate(flops=int(us * 1e3 * 4000), bytes_accessed=1, transcendentals=0)


def small(body, outs, mib, *operands, scratch=(), specs=None):
    return pl.pallas_call(
        body,
        out_shape=outs,
        in_specs=specs or in_vmem(len(operands)),
        out_specs=jax.tree.map(lambda _: pl.BlockSpec(memory_space=pltpu.VMEM), outs),
        scratch_shapes=scratch,
        compiler_params=params(mib),
        cost_estimate=cost(1.0),
    )(*operands)


def merged(blocks, mine, start, theirs, high, inv, moved, outs):
    operands = [*blocks, high, inv, *moved]
    count = len(operands)
    aliases = {}
    specs = in_vmem(count)
    if outs is None:
        outs = ()

        def body(*refs):
            merge_kernel(mine, start, theirs, *refs[:count], None, None, *refs[count:])
    else:
        aliases = {count: 0, count + 1: 1}
        specs = specs + [ANY, ANY]
        body = functools.partial(merge_kernel, mine, start, theirs)
    n, rows = len(mine), blocks[0].shape[0]
    copies = 2 * (n + sum(len(pair) for pair, _ in theirs))
    return pl.pallas_call(
        body,
        out_shape=(OUT, OUT, jax.ShapeDtypeStruct((n, rows, WIDE), jnp.bfloat16)),
        in_specs=specs,
        out_specs=(ANY, ANY, pl.BlockSpec(memory_space=pltpu.VMEM)),
        scratch_shapes=[pltpu.SemaphoreType.DMA((copies,))],
        input_output_aliases=aliases,
        compiler_params=params(14),
        cost_estimate=cost(1.5),
    )(*operands, *outs)


def placed(theirs, moved, outs):
    n = len(moved)
    copies = 2 * sum(len(pair) for pair, _ in theirs)
    return pl.pallas_call(
        functools.partial(place_kernel, theirs),
        out_shape=(OUT, OUT),
        in_specs=in_vmem(n) + [ANY, ANY],
        out_specs=(ANY, ANY),
        scratch_shapes=[pltpu.SemaphoreType.DMA((copies,))],
        input_output_aliases={n: 0, n + 1: 1},
        compiler_params=params(10),
        cost_estimate=cost(1.0),
    )(*moved, *outs)


def program(weight_gate, low_gate, high_gate, weight_up, low_up, high_up, norm_gain):
    hbm = pl.BlockSpec(memory_space=pltpu.HBM)
    shape = jax.ShapeDtypeStruct
    a_block = shape((ROWS, FULL), jnp.bfloat16)
    a_sum = shape((1, WIDE), jnp.float32)
    block, high = small(
        pack_kernel,
        (a_block, shape((2 * RANK, WIDE), jnp.bfloat16)),
        6,
        *(
            pltpu.with_memory_space_constraint(a, pltpu.HBM)
            for a in (
                weight_gate,
                weight_up,
                low_gate.T,
                low_up.T,
                norm_gain.reshape(1, ROWS),
                high_gate,
                high_up,
            )
        ),
        specs=[hbm] * 7,
        scratch=[
            pltpu.VMEM((2, RANK, ROWS), jnp.bfloat16),
            pltpu.VMEM((1, ROWS), jnp.float32),
            pltpu.VMEM((128, 128), jnp.float32),
            pltpu.SemaphoreType.DMA((7,)),
        ],
    )
    held = {(0, 0): block}
    for step in (1, -1):
        held[-step, 0] = sent(block, FIRST[step])
    for step in (1, -1):
        held[0, -step] = sent(block, SECOND[step])

    total = small(sums_kernel, a_sum, 6, block, high)
    for along, bits in ((SECOND, (3, 1)), (FIRST, (1, 3))):
        others = [sent(total, along[d]) for d in (1, -1, 2)]
        body = functools.partial(ring_kernel, bits)
        total = small(body, a_sum, 2, total, *others)
    twin = sent(total, SIDE)
    factor, inv = small(factor_kernel, (a_sum, a_sum), 2, total, twin)

    def halves(a, b):
        shapes = (shape((TOP, FULL), jnp.bfloat16), shape((ROWS - TOP, FULL), jnp.bfloat16))
        return small(halves_kernel, shapes, 6, a, b)

    top, bottom = halves(held[-1, 0], held[1, 0])
    top, bottom = sent(top, FIRST[1]), sent(bottom, FIRST[-1])
    held[2, 0] = small(joined_kernel, a_block, 6, top, bottom)

    for step, order in ((1, (-1, 1, 2)), (-1, (1, -1, 2))):
        for f in order:
            held[f, -step] = sent(held[f, 0], SECOND[step])
    held[0, 2] = sent(held[0, -1], SECOND[1])
    held[1, 2] = sent(held[1, 1], SECOND[-1])
    pieces = []
    for step, f in ((1, -1), (-1, 2)):
        block = held[f, -step]
        top, bottom = halves(block, block)
        pieces.append([sent(p, SECOND[step]) for p in (top, bottom)])

    pairs = (
        ((0, 0), (-1, 0)),
        ((0, -1), (0, 1)),
        ((1, 0), (2, 0)),
        ((-1, -1), (1, 1)),
        ((1, -1), (-1, 1)),
        ((2, -1), (2, 1)),
        ((0, 2), (1, 2)),
    )
    last = ((-1, 2), (2, 2))
    work = [([held[p] for p in pair], pair, 0) for pair in pairs]
    work += [(piece, last, start) for piece, start in zip(zip(*pieces), (0, TOP))]
    late = {k: (k - 2,) for k in range(2, len(pairs))}
    late[len(pairs)] = (len(pairs) - 2, len(pairs) - 1)
    outs, moved = None, []
    for k, (blocks, pair, start) in enumerate(work):
        theirs = [work[j][1:] for j in late.get(k, ())]
        arrived = [moved[j] for j in late.get(k, ())]
        *outs, ready = merged(blocks, pair, start, theirs, high, inv, arrived, outs)
        moved.append(sent(ready, SIDE))
    theirs = [work[j][1:] for j in (-2, -1)]
    ready_gate, ready_up = placed(theirs, moved[-2:], outs)
    factor = factor.reshape(WIDE)
    return ready_gate, ready_up, factor[:HALF], factor[HALF:]


def solution(mesh):
    in_specs = (
        P("shard", "tp"),
        P("shard", None),
        P(None, "tp"),
        P("shard", "tp"),
        P("shard", None),
        P(None, "tp"),
        P("shard"),
    )
    out_specs = (P(None, "tp"), P(None, "tp"), P("tp"), P("tp"))
    return jax.shard_map(program, mesh=mesh, in_specs=in_specs, out_specs=out_specs, check_vma=False)
```

```python
import functools

import jax
import jax.numpy as jnp
from jax import lax
from jax.experimental import pallas as pl
from jax.experimental.pallas import tpu as pltpu
from jax.sharding import PartitionSpec as P


ROWS = 80
HALF = 2432
WIDE = 2 * HALF
FULL = WIDE + 128
TILE = 256
KIB = 1024
RANK = 32
CUT = 2560
TOP = 48
mix_rate = 2.0


def shard_of(y, x, c):
    return ((y % 4) * 4 + x % 4) * 2 + c


def hops(core0, core1, flip=0):
    step = (core0, core1)
    return [
        (shard_of(y, x, c), shard_of(y + step[c][0], x + step[c][1], c ^ flip))
        for y in range(4)
        for x in range(4)
        for c in range(2)
    ]


FIRST = {d: hops((0, d), (d, 0)) for d in (1, -1, 2)}
SECOND = {d: hops((d, 0), (0, d)) for d in (1, -1, 2)}
SIDE = hops((0, 0), (0, 0), 1)


def source(first, second, flip):
    me = lax.axis_index("shard")
    core, x, y = (me & 1) ^ flip, (me >> 1) & 3, me >> 3
    sx = (x + jnp.where(core == 0, first, second)) & 3
    sy = (y + jnp.where(core == 0, second, first)) & 3
    return ((sy << 2) + sx) * 2 + core


def sent(array, pairs):
    return lax.ppermute(array, "shard", pairs)


def in_vmem(n):
    return [pl.BlockSpec(memory_space=pltpu.VMEM)] * n


def pack_kernel(gate, up, low_gate_t, low_up_t, gain, high_gate, high_up, block, high, low_v, gain_v, side, sems):
    moves = (
        (low_gate_t, low_v.at[0]),
        (low_up_t, low_v.at[1]),
        (gain, gain_v),
        (gate, block.at[:, pl.ds(0, HALF)]),
        (up, block.at[:, pl.ds(HALF, HALF)]),
        (high_gate, high.at[pl.ds(0, RANK), pl.ds(0, HALF)]),
        (high_up, high.at[pl.ds(RANK, RANK), pl.ds(HALF, HALF)]),
    )
    copies = [pltpu.make_async_copy(src, dst, sems.at[k]) for k, (src, dst) in enumerate(moves)]
    for copy in copies:
        copy.start()
    high[0:RANK, HALF:] = jnp.zeros((RANK, HALF), jnp.bfloat16)
    high[RANK : 2 * RANK, :HALF] = jnp.zeros((RANK, HALF), jnp.bfloat16)
    side[...] = jnp.zeros_like(side)
    for copy in copies[:3]:
        copy.wait()
    g = gain_v[...]
    hi = g.astype(jnp.bfloat16).astype(jnp.float32)
    mid = (g - hi).astype(jnp.bfloat16).astype(jnp.float32)
    side[0:32, 0:ROWS] = low_v[0].astype(jnp.float32) * mix_rate
    side[32:64, 0:ROWS] = low_v[1].astype(jnp.float32) * mix_rate
    side[64:65, 0:ROWS] = hi
    side[65:66, 0:ROWS] = mid
    side[66:67, 0:ROWS] = g - hi - mid
    block[:, WIDE:] = side[...].T[0:ROWS].astype(jnp.bfloat16)
    for copy in copies[3:]:
        copy.wait()


def gain_of(extra):
    row = lax.broadcasted_iota(jnp.int32, (128, 128), 0)
    ones = jnp.where((row >= 64) & (row < 67), 1.0, 0.0).astype(jnp.bfloat16)
    g = jnp.dot(extra, ones, preferred_element_type=jnp.float32)
    return jnp.concatenate([g, g], axis=1)


def sums_kernel(block, high, sums):
    extra = block[:, WIDE:]
    gain = gain_of(extra)
    for j in range(WIDE // TILE):
        cols = pl.ds(j * TILE, TILE)
        v = block[:, cols].astype(jnp.float32) + jnp.dot(
            extra[:, :64], high[:, cols], preferred_element_type=jnp.float32
        )
        v = v * gain
        sums[:, cols] = jnp.sum(v * v, axis=0, keepdims=True)


def ring_kernel(bits, own, plus, minus, far, total):
    me = lax.axis_index("shard")
    bit = jnp.where((me & 1) == 0, bits[0], bits[1])
    even = ((me >> bit) & 1) == 0
    p, m = plus[...], minus[...]
    partner, other = jnp.where(even, m, p), jnp.where(even, p, m)
    total[...] = (own[...] + partner) + (other + far[...])


def factor_kernel(mine, theirs, factor, inv):
    root = jnp.sqrt(mine[...] + theirs[...])
    factor[...] = root
    inv[...] = 1.0 / root


def halves_kernel(a, b, left, right):
    left[...] = a[:, :CUT]
    right[...] = b[:, CUT:]


def joined_kernel(left, right, block):
    block[:, :CUT] = left[...]
    block[:, CUT:] = right[...]


def pieces_kernel(block, top, bottom):
    top[...] = block[:TOP]
    bottom[...] = block[TOP:]


def placer(outs, sems, copies):
    def send(src, at, start, flip, h):
        count = src.shape[0]
        row = pl.multiple_of(source(*at, flip) * ROWS + start, 16)
        copy = pltpu.make_async_copy(
            src.at[:, pl.ds(h * HALF, HALF)],
            outs[h].at[pl.ds(row, count), :],
            sems.at[len(copies)],
        )
        copy.start()
        copies.append(copy)

    return send


def merge_kernel(mine, start, flip, theirs, *refs):
    n, place = len(mine), len(theirs)
    blocks, refs = refs[:n], refs[n:]
    high, inv = refs[0], refs[1]
    moved, refs = refs[2 : 2 + place], refs[2 + place :]
    out_gate, out_up, ready, sems = refs[2:]
    count = ready.shape[1]
    copies = []
    send = placer((out_gate, out_up), sems, copies)
    for (pair, first), ref in zip(theirs, moved):
        for k, at in enumerate(pair):
            for h in range(2):
                send(ref.at[k], at, first, 1, h)
    extra = jnp.concatenate([b[:, WIDE:] for b in blocks], axis=0)
    gain = gain_of(extra)
    for j in range(WIDE // TILE):
        cols = pl.ds(j * TILE, TILE)
        low_rank = jnp.dot(extra[:, :64], high[:, cols], preferred_element_type=jnp.float32)
        scale = inv[:, cols]
        for k in range(n):
            rows = slice(k * count, (k + 1) * count)
            v = blocks[k][:, cols].astype(jnp.float32) + low_rank[rows]
            ready[k, :, cols] = (v * gain[rows] * scale).astype(jnp.bfloat16)
        if j == HALF // TILE:
            for k in range(n):
                send(ready.at[k], mine[k], start, flip, 0)
    for k in range(n):
        send(ready.at[k], mine[k], start, flip, 1)
    for copy in copies:
        copy.wait()


OUT = jax.ShapeDtypeStruct((32 * ROWS, HALF), jnp.bfloat16)
ANY = pl.BlockSpec(memory_space=pl.ANY)


def params(mib):
    return pltpu.CompilerParams(vmem_limit_bytes=int(mib * KIB * KIB))


def cost(us):
    return pl.CostEstimate(flops=int(us * 1e3 * 4000), bytes_accessed=1, transcendentals=0)


def small(body, outs, mib, *operands, scratch=(), specs=None):
    return pl.pallas_call(
        body,
        out_shape=outs,
        in_specs=specs or in_vmem(len(operands)),
        out_specs=jax.tree.map(lambda _: pl.BlockSpec(memory_space=pltpu.VMEM), outs),
        scratch_shapes=scratch,
        compiler_params=params(mib),
        cost_estimate=cost(1.0),
    )(*operands)


def merged(blocks, mine, start, flip, theirs, high, inv, moved, outs, hand_over):
    operands = [*blocks, high, inv, *moved]
    count = len(operands)
    aliases = {}
    specs = in_vmem(count)
    if outs is None:
        outs = ()

        def body(*refs):
            merge_kernel(mine, start, flip, theirs, *refs[:count], None, None, *refs[count:])
    else:
        aliases = {count: 0, count + 1: 1}
        specs = specs + [ANY, ANY]
        body = functools.partial(merge_kernel, mine, start, flip, theirs)
    n, rows = len(mine), blocks[0].shape[0]
    ready = (n, rows, WIDE)
    kept = () if hand_over else (pltpu.VMEM(ready, jnp.bfloat16),)
    given = (jax.ShapeDtypeStruct(ready, jnp.bfloat16),) if hand_over else ()
    copies = 2 * (n + sum(len(pair) for pair, _ in theirs))
    return pl.pallas_call(
        body,
        out_shape=(OUT, OUT, *given),
        in_specs=specs,
        out_specs=(ANY, ANY, *in_vmem(len(given))),
        scratch_shapes=[*kept, pltpu.SemaphoreType.DMA((copies,))],
        input_output_aliases=aliases,
        compiler_params=params(14),
        cost_estimate=cost(1.5),
    )(*operands, *outs)


def program(weight_gate, low_gate, high_gate, weight_up, low_up, high_up, norm_gain):
    hbm = pl.BlockSpec(memory_space=pltpu.HBM)
    shape = jax.ShapeDtypeStruct
    a_block = shape((ROWS, FULL), jnp.bfloat16)
    a_sum = shape((1, WIDE), jnp.float32)
    block, high = small(
        pack_kernel,
        (a_block, shape((2 * RANK, WIDE), jnp.bfloat16)),
        6,
        *(
            pltpu.with_memory_space_constraint(a, pltpu.HBM)
            for a in (
                weight_gate,
                weight_up,
                low_gate.T,
                low_up.T,
                norm_gain.reshape(1, ROWS),
                high_gate,
                high_up,
            )
        ),
        specs=[hbm] * 7,
        scratch=[
            pltpu.VMEM((2, RANK, ROWS), jnp.bfloat16),
            pltpu.VMEM((1, ROWS), jnp.float32),
            pltpu.VMEM((128, 128), jnp.float32),
            pltpu.SemaphoreType.DMA((7,)),
        ],
    )
    held = {(0, 0): block}
    for step in (1, -1):
        held[-step, 0] = sent(block, FIRST[step])
    for step in (1, -1):
        held[0, -step] = sent(block, SECOND[step])

    total = small(sums_kernel, a_sum, 6, block, high)
    for along, bits in ((SECOND, (3, 1)), (FIRST, (1, 3))):
        others = [sent(total, along[d]) for d in (1, -1, 2)]
        body = functools.partial(ring_kernel, bits)
        total = small(body, a_sum, 2, total, *others)
    twin = sent(total, SIDE)
    factor, inv = small(factor_kernel, (a_sum, a_sum), 2, total, twin)

    left, right = small(
        halves_kernel,
        (shape((ROWS, CUT), jnp.bfloat16), shape((ROWS, FULL - CUT), jnp.bfloat16)),
        6,
        held[-1, 0],
        held[1, 0],
    )
    left, right = sent(left, FIRST[1]), sent(right, FIRST[-1])
    held[2, 0] = small(joined_kernel, a_block, 6, left, right)

    for step, order in ((1, (-1, 1, 2)), (-1, (1, -1, 2))):
        for f in order:
            held[f, -step] = sent(held[f, 0], SECOND[step])
    held[0, 2] = sent(held[0, -1], SECOND[1])
    held[1, 2] = sent(held[1, 1], SECOND[-1])
    tops, bottoms = [], []
    shapes = (shape((TOP, FULL), jnp.bfloat16), shape((ROWS - TOP, FULL), jnp.bfloat16))
    for step, f in ((1, -1), (-1, 2)):
        top, bottom = small(pieces_kernel, shapes, 6, held[f, -step])
        tops.append(sent(top, SECOND[step]))
        bottoms.append(sent(bottom, SECOND[step]))
    twins = [sent(bottom, SIDE) for bottom in bottoms]

    pairs = (
        ((0, 0), (-1, 0)),
        ((0, -1), (0, 1)),
        ((1, 0), (2, 0)),
        ((-1, -1), (1, 1)),
        ((1, -1), (-1, 1)),
        ((2, -1), (2, 1)),
        ((0, 2), (1, 2)),
    )
    last = ((-1, 2), (2, 2))
    work = [([held[p] for p in pair], pair, 0, 0) for pair in pairs]
    work += [(tops, last, 0, 0), (bottoms, last, TOP, 0), (twins, last, TOP, 1)]
    late = {k: (k - 2,) for k in range(2, 7)} | {7: (5, 6), 9: (7,)}
    outs, moved = None, []
    for k, (blocks, pair, start, flip) in enumerate(work):
        theirs = [work[j][1:3] for j in late.get(k, ())]
        arrived = [moved[j] for j in late.get(k, ())]
        hand_over = k < 8
        results = merged(blocks, pair, start, flip, theirs, high, inv, arrived, outs, hand_over)
        outs = results[:2]
        if hand_over:
            moved.append(sent(results[2], SIDE))
    ready_gate, ready_up = outs
    factor = factor.reshape(WIDE)
    return ready_gate, ready_up, factor[:HALF], factor[HALF:]


def solution(mesh):
    in_specs = (
        P("shard", "tp"),
        P("shard", None),
        P(None, "tp"),
        P("shard", "tp"),
        P("shard", None),
        P(None, "tp"),
        P("shard"),
    )
    out_specs = (P(None, "tp"), P(None, "tp"), P("tp"), P("tp"))
    return jax.shard_map(program, mesh=mesh, in_specs=in_specs, out_specs=out_specs, check_vma=False)
```

```python
import functools

import jax
import jax.numpy as jnp
from jax import lax
from jax.experimental import pallas as pl
from jax.experimental.pallas import tpu as pltpu
from jax.sharding import PartitionSpec as P


ROWS = 80
HALF = 2432
WIDE = 2 * HALF
FULL = WIDE + 128
TILE = 256
KIB = 1024
RANK = 32
CUT = 2560
TOP = 48
mix_rate = 2.0


def shard_of(y, x, c):
    return ((y % 4) * 4 + x % 4) * 2 + c


def hops(core0, core1, flip=0):
    step = (core0, core1)
    return [
        (shard_of(y, x, c), shard_of(y + step[c][0], x + step[c][1], c ^ flip))
        for y in range(4)
        for x in range(4)
        for c in range(2)
    ]


FIRST = {d: hops((0, d), (d, 0)) for d in (1, -1, 2)}
SECOND = {d: hops((d, 0), (0, d)) for d in (1, -1, 2)}
SIDE = hops((0, 0), (0, 0), 1)


def source(first, second, flip):
    me = lax.axis_index("shard")
    core, x, y = (me & 1) ^ flip, (me >> 1) & 3, me >> 3
    sx = (x + jnp.where(core == 0, first, second)) & 3
    sy = (y + jnp.where(core == 0, second, first)) & 3
    return ((sy << 2) + sx) * 2 + core


def sent(array, pairs):
    return lax.ppermute(array, "shard", pairs)


def in_vmem(n):
    return [pl.BlockSpec(memory_space=pltpu.VMEM)] * n


def pack_kernel(gate, up, low_gate_t, low_up_t, gain, high_gate, high_up, block, high, low_v, gain_v, side, sems):
    moves = (
        (low_gate_t, low_v.at[0]),
        (low_up_t, low_v.at[1]),
        (gain, gain_v),
        (gate, block.at[:, pl.ds(0, HALF)]),
        (up, block.at[:, pl.ds(HALF, HALF)]),
        (high_gate, high.at[pl.ds(0, RANK), pl.ds(0, HALF)]),
        (high_up, high.at[pl.ds(RANK, RANK), pl.ds(HALF, HALF)]),
    )
    copies = [pltpu.make_async_copy(src, dst, sems.at[k]) for k, (src, dst) in enumerate(moves)]
    for copy in copies:
        copy.start()
    high[0:RANK, HALF:] = jnp.zeros((RANK, HALF), jnp.bfloat16)
    high[RANK : 2 * RANK, :HALF] = jnp.zeros((RANK, HALF), jnp.bfloat16)
    side[...] = jnp.zeros_like(side)
    for copy in copies[:3]:
        copy.wait()
    g = gain_v[...]
    hi = g.astype(jnp.bfloat16).astype(jnp.float32)
    mid = (g - hi).astype(jnp.bfloat16).astype(jnp.float32)
    side[0:32, 0:ROWS] = low_v[0].astype(jnp.float32) * mix_rate
    side[32:64, 0:ROWS] = low_v[1].astype(jnp.float32) * mix_rate
    side[64:65, 0:ROWS] = hi
    side[65:66, 0:ROWS] = mid
    side[66:67, 0:ROWS] = g - hi - mid
    block[:, WIDE:] = side[...].T[0:ROWS].astype(jnp.bfloat16)
    for copy in copies[3:]:
        copy.wait()


def gain_of(extra):
    row = lax.broadcasted_iota(jnp.int32, (128, 128), 0)
    ones = jnp.where((row >= 64) & (row < 67), 1.0, 0.0).astype(jnp.bfloat16)
    g = jnp.dot(extra, ones, preferred_element_type=jnp.float32)
    return jnp.concatenate([g, g], axis=1)


def sums_kernel(block, high, sums):
    extra = block[:, WIDE:]
    gain = gain_of(extra)
    for j in range(WIDE // TILE):
        cols = pl.ds(j * TILE, TILE)
        v = block[:, cols].astype(jnp.float32) + jnp.dot(
            extra[:, :64], high[:, cols], preferred_element_type=jnp.float32
        )
        v = v * gain
        sums[:, cols] = jnp.sum(v * v, axis=0, keepdims=True)


def ring_kernel(bits, own, plus, minus, far, total):
    me = lax.axis_index("shard")
    bit = jnp.where((me & 1) == 0, bits[0], bits[1])
    even = ((me >> bit) & 1) == 0
    p, m = plus[...], minus[...]
    partner, other = jnp.where(even, m, p), jnp.where(even, p, m)
    total[...] = (own[...] + partner) + (other + far[...])


def factor_kernel(mine, theirs, factor, inv):
    root = jnp.sqrt(mine[...] + theirs[...])
    factor[...] = root
    inv[...] = 1.0 / root


def halves_kernel(a, b, left, right):
    left[...] = a[:, :CUT]
    right[...] = b[:, CUT:]


def joined_kernel(left, right, block):
    block[:, :CUT] = left[...]
    block[:, CUT:] = right[...]


def placer(outs, sems, copies):
    def send(src, at, start, flip, h):
        count = src.shape[0]
        row = pl.multiple_of(source(*at, flip) * ROWS + start, 16)
        copy = pltpu.make_async_copy(
            src.at[:, pl.ds(h * HALF, HALF)],
            outs[h].at[pl.ds(row, count), :],
            sems.at[len(copies)],
        )
        copy.start()
        copies.append(copy)

    return send


def merge_kernel(mine, theirs, pieces, *refs):
    n, place = len(mine), len(theirs)
    blocks, refs = refs[:n], refs[n:]
    high, inv = refs[0], refs[1]
    moved, refs = refs[2 : 2 + place], refs[2 + place :]
    out_gate, out_up, ready = refs[2:5]
    onward, sems = refs[5:-1], refs[-1]
    copies = []
    send = placer((out_gate, out_up), sems, copies)
    for group, ref in zip(theirs, moved):
        for k, at in enumerate(group):
            for h in range(2):
                send(ref.at[k], at, 0, 1, h)
    extra = jnp.concatenate([b[:, WIDE:] for b in blocks], axis=0)
    gain = gain_of(extra)
    for j in range(WIDE // TILE):
        cols = pl.ds(j * TILE, TILE)
        low_rank = jnp.dot(extra[:, :64], high[:, cols], preferred_element_type=jnp.float32)
        scale = inv[:, cols]
        for k in range(n):
            rows = slice(k * ROWS, (k + 1) * ROWS)
            v = blocks[k][:, cols].astype(jnp.float32) + low_rank[rows]
            v = (v * gain[rows] * scale).astype(jnp.bfloat16)
            ready[k, :, cols] = v
            for (of, start, count), ref in zip(pieces, onward):
                if of == k:
                    ref[:, cols] = v[start : start + count]
        if j == HALF // TILE:
            for k in range(n):
                send(ready.at[k], mine[k], 0, 0, 0)
    for k in range(n):
        send(ready.at[k], mine[k], 0, 0, 1)
    for copy in copies:
        copy.wait()


def place_kernel(items, groups, *refs):
    arrays, refs = refs[: len(items)], refs[len(items) :]
    moved, refs = refs[: len(groups)], refs[len(groups) + 2 :]
    copies = []
    send = placer(refs[:2], refs[2], copies)
    for item, ref in zip(items, arrays):
        for h in range(2):
            send(ref, *item, h)
    for group, ref in zip(groups, moved):
        for k, at in enumerate(group):
            for h in range(2):
                send(ref.at[k], at, 0, 1, h)
    for copy in copies:
        copy.wait()


OUT = jax.ShapeDtypeStruct((32 * ROWS, HALF), jnp.bfloat16)
ANY = pl.BlockSpec(memory_space=pl.ANY)


def params(mib):
    return pltpu.CompilerParams(vmem_limit_bytes=int(mib * KIB * KIB))


def cost(us):
    return pl.CostEstimate(flops=int(us * 1e3 * 4000), bytes_accessed=1, transcendentals=0)


def small(body, outs, mib, *operands, scratch=(), specs=None):
    return pl.pallas_call(
        body,
        out_shape=outs,
        in_specs=specs or in_vmem(len(operands)),
        out_specs=jax.tree.map(lambda _: pl.BlockSpec(memory_space=pltpu.VMEM), outs),
        scratch_shapes=scratch,
        compiler_params=params(mib),
        cost_estimate=cost(1.0),
    )(*operands)


def merged(blocks, mine, theirs, pieces, high, inv, moved, outs):
    operands = [*blocks, high, inv, *moved]
    count = len(operands)
    aliases = {}
    specs = in_vmem(count)
    if outs is None:
        outs = ()

        def body(*refs):
            merge_kernel(mine, theirs, pieces, *refs[:count], None, None, *refs[count:])
    else:
        aliases = {count: 0, count + 1: 1}
        specs = specs + [ANY, ANY]
        body = functools.partial(merge_kernel, mine, theirs, pieces)
    n = len(mine)
    onward = [jax.ShapeDtypeStruct((rows, WIDE), jnp.bfloat16) for _, _, rows in pieces]
    copies = 2 * (n + sum(len(group) for group in theirs))
    return pl.pallas_call(
        body,
        out_shape=(OUT, OUT, jax.ShapeDtypeStruct((n, ROWS, WIDE), jnp.bfloat16), *onward),
        in_specs=specs,
        out_specs=(ANY, ANY, *in_vmem(1 + len(onward))),
        scratch_shapes=[pltpu.SemaphoreType.DMA((copies,))],
        input_output_aliases=aliases,
        compiler_params=params(14),
        cost_estimate=cost(1.5),
    )(*operands, *outs)


def placed(items, arrays, groups, moved, outs):
    n = len(arrays) + len(moved)
    copies = 2 * (len(items) + sum(len(group) for group in groups))
    return pl.pallas_call(
        functools.partial(place_kernel, items, groups),
        out_shape=(OUT, OUT),
        in_specs=in_vmem(n) + [ANY, ANY],
        out_specs=(ANY, ANY),
        scratch_shapes=[pltpu.SemaphoreType.DMA((copies,))],
        input_output_aliases={n: 0, n + 1: 1},
        compiler_params=params(14),
        cost_estimate=cost(1.0),
    )(*arrays, *moved, *outs)


def program(weight_gate, low_gate, high_gate, weight_up, low_up, high_up, norm_gain):
    hbm = pl.BlockSpec(memory_space=pltpu.HBM)
    shape = jax.ShapeDtypeStruct
    a_block = shape((ROWS, FULL), jnp.bfloat16)
    a_sum = shape((1, WIDE), jnp.float32)
    block, high = small(
        pack_kernel,
        (a_block, shape((2 * RANK, WIDE), jnp.bfloat16)),
        6,
        *(
            pltpu.with_memory_space_constraint(a, pltpu.HBM)
            for a in (
                weight_gate,
                weight_up,
                low_gate.T,
                low_up.T,
                norm_gain.reshape(1, ROWS),
                high_gate,
                high_up,
            )
        ),
        specs=[hbm] * 7,
        scratch=[
            pltpu.VMEM((2, RANK, ROWS), jnp.bfloat16),
            pltpu.VMEM((1, ROWS), jnp.float32),
            pltpu.VMEM((128, 128), jnp.float32),
            pltpu.SemaphoreType.DMA((7,)),
        ],
    )
    held = {(0, 0): block}
    for step in (1, -1):
        held[-step, 0] = sent(block, FIRST[step])
    for step in (1, -1):
        held[0, -step] = sent(block, SECOND[step])

    total = small(sums_kernel, a_sum, 6, block, high)
    for along, bits in ((SECOND, (3, 1)), (FIRST, (1, 3))):
        others = [sent(total, along[d]) for d in (1, -1, 2)]
        body = functools.partial(ring_kernel, bits)
        total = small(body, a_sum, 2, total, *others)
    twin = sent(total, SIDE)
    factor, inv = small(factor_kernel, (a_sum, a_sum), 2, total, twin)

    left, right = small(
        halves_kernel,
        (shape((ROWS, CUT), jnp.bfloat16), shape((ROWS, FULL - CUT), jnp.bfloat16)),
        6,
        held[-1, 0],
        held[1, 0],
    )
    left, right = sent(left, FIRST[1]), sent(right, FIRST[-1])
    held[2, 0] = small(joined_kernel, a_block, 6, left, right)

    for step, order in ((1, (-1, 1, 2)), (-1, (1, -1, 2))):
        for f in order:
            held[f, -step] = sent(held[f, 0], SECOND[step])
    pairs = (
        ((0, 0), (-1, 0)),
        ((0, -1), (0, 1)),
        ((1, 0), (2, 0)),
        ((-1, -1), (1, 1)),
        ((1, -1), (-1, 1)),
        ((2, -1), (2, 1)),
    )
    whole, top, bottom = (0, ROWS), (0, TOP), (TOP, ROWS - TOP)
    onward = {
        1: (("on1_0", 1, 0, *whole),),
        3: (
            ("on-1_1", -1, 1, *whole),
            ("on1_-1t", 1, 0, *top),
            ("on1_-1b", 1, 0, *bottom),
        ),
        5: (("on-1_2t", -1, 1, *top), ("on-1_2b", -1, 1, *bottom)),
    }
    outs, moved, came = None, [], {}
    for k, pair in enumerate(pairs):
        late = [k - 2] if k >= 2 else []
        steps = onward.get(k, ())
        results = merged(
            [held[p] for p in pair],
            pair,
            [pairs[j] for j in late],
            [step[2:] for step in steps],
            high,
            inv,
            [moved[j] for j in late],
            outs,
        )
        outs = results[:2]
        moved.append(sent(results[2], SIDE))
        for step, rows in zip(steps, results[3:]):
            came[step[0]] = sent(rows, SECOND[step[1]])

    places = {
        "on1_0": ((0, 2), 0),
        "on-1_1": ((1, 2), 0),
        "on1_-1t": ((-1, 2), 0),
        "on-1_2t": ((2, 2), 0),
        "on1_-1b": ((-1, 2), TOP),
        "on-1_2b": ((2, 2), TOP),
    }
    twin = {name: sent(came[name], SIDE) for name in places}
    names = tuple(places)

    def put(outs, own, twins, sides):
        items = [(*places[n], 0) for n in own] + [(*places[n], 1) for n in twins]
        arrays = [came[n] for n in own] + [twin[n] for n in twins]
        groups = [pairs[j] for j in sides]
        return placed(items, arrays, groups, [moved[j] for j in sides], outs)

    outs = put(outs, names[:2], (), (4, 5))
    outs = put(outs, names[2:4], names[:2], ())
    outs = put(outs, names[4:], names[2:4], ())
    ready_gate, ready_up = put(outs, (), names[4:], ())
    factor = factor.reshape(WIDE)
    return ready_gate, ready_up, factor[:HALF], factor[HALF:]


def solution(mesh):
    in_specs = (
        P("shard", "tp"),
        P("shard", None),
        P(None, "tp"),
        P("shard", "tp"),
        P("shard", None),
        P(None, "tp"),
        P("shard"),
    )
    out_specs = (P(None, "tp"), P(None, "tp"), P("tp"), P("tp"))
    return jax.shard_map(program, mesh=mesh, in_specs=in_specs, out_specs=out_specs, check_vma=False)
```
